32 devices in a mesh: fsdp: 8 (over y, x, core), seq: 4 (over z).
Axes of the slice: x: 2, y: 2, z: 4, core: 2. Of those that a mesh axis runs over, the one named last changes fastest.
Arguments:
- inputs: bfloat16 [8192, 1536], P(('fsdp', 'seq')), may hold values from -6 to 6
- norm_attn: bfloat16 [1536], P('fsdp'), may hold values from 0.5 to 1.5
- w_proj: bfloat16 [1536, 6144], P('fsdp'), may hold values from -0.15625 to 0.15625
- w_small: bfloat16 [1536, 72], P('fsdp'), may hold values from -0.15625 to 0.15625
- forget_bias: float32 [24], replicated, may hold values from 3 to 9
- qk_gain: bfloat16 [2, 64], replicated, may hold values from 0.5 to 1.5
- w_out: bfloat16 [1536, 1536], P('fsdp'), may hold values from -0.625 to 0.625
- norm_ffn: bfloat16 [1536], P('fsdp'), may hold values from 0.5 to 1.5
- w_in: bfloat16 [1536, 8192], P('fsdp'), may hold values from -0.15625 to 0.15625
- w_down: bfloat16 [4096, 1536], P('fsdp'), may hold values from -0.09375 to 0.09375
- cotangent: bfloat16 [8192, 1536], P(('fsdp', 'seq')), may hold values from -6 to 6
Outputs:
- output: bfloat16 [8192, 1536], P(('fsdp', 'seq'))
- grad_inputs: float32 [8192, 1536], P(('fsdp', 'seq'))
- grad_norm_attn: float32 [1536], P('fsdp')
- grad_proj: float32 [1536, 6144], P('fsdp')
- grad_small: float32 [1536, 72], P('fsdp')
- grad_forget_bias: float32 [24], replicated
- grad_qk_gain: float32 [2, 64], replicated
- grad_out: float32 [1536, 1536], P('fsdp')
- grad_norm_ffn: float32 [1536], P('fsdp')
- grad_in: float32 [1536, 8192], P('fsdp')
- grad_down: float32 [4096, 1536], P('fsdp')
The draws below stay inside these ranges and needn't reach their ends.
All inputs are finite; a program needn't handle non-finite values.
Results may differ from the reference program's by a relative error of at most 0.02.
Values may be sent and summed in bfloat16 or wider, within the bound.
No kernel may reach another device: no remote copies, remote signals or barrier semaphores. Data moves between devices by JAX's collectives and lax.ppermute only.
A program may use at most 320 MiB of HBM per device.

```python
import jax
import jax.numpy as jnp
from jax import lax

D = 1536
H = 24
HD = 64
FF = 4096
SEQ_ROWS = 256
QBLOCK = 512
TOKENS = 8192
N_SEQ = 4


def steps_of(rng, extent, split, least, top_value):
    def one(axis_at, shards_of):
        steps = jax.random.uniform(jax.random.fold_in(jax.random.fold_in(rng, 6), axis_at), (shards_of,), jnp.float32, least / len(split), top_value / len(split))
        return jnp.repeat(jnp.exp(steps), extent[axis_at] // shards_of).reshape((-1,) + (1,) * (len(extent) - axis_at - 1))

    factor_of = one(*split[0])
    for cut in split[1:]:
        factor_of = factor_of * one(*cut)
    return factor_of


def normal_values(rng, shape, scale, most, split=(), kind=jnp.bfloat16):
    drawn = jax.random.normal(rng, shape, jnp.float32) * scale
    if len(split) > 0:
        drawn = steps_of(rng, shape, split, -0.22, 0.18) * drawn
    return jnp.clip(drawn, min=-most, max=most).astype(kind)


def setup_inputs(seed: int = 0) -> dict:
    key_of = jax.random.split(jax.random.key(seed), 12)
    return {
        "inputs": normal_values(key_of[0], (TOKENS, D), 1.0, 6.0, ((0, 32),)),
        "norm_attn": jnp.clip(1.0 + 0.1 * jax.random.normal(key_of[1], (D,), jnp.float32), 0.5, 1.5).astype(jnp.bfloat16),
        "w_proj": normal_values(key_of[2], (D, 4 * D), D ** -0.5, 0.15625, ((0, 8),)),
        "w_small": normal_values(key_of[3], (D, 3 * H), D ** -0.5, 0.15625, ((0, 8),)),
        "forget_bias": jnp.clip(jax.random.uniform(key_of[4], (H,), jnp.float32, 3.0, 9.0), 3.0, 9.0),
        "qk_gain": jnp.clip(1.0 + 0.1 * jax.random.normal(key_of[5], (2, HD), jnp.float32), 0.5, 1.5).astype(jnp.bfloat16),
        "w_out": normal_values(key_of[6], (D, D), (D // 16) ** -0.5, 0.625, ((0, 8),)),
        "norm_ffn": jnp.clip(1.0 + 0.1 * jax.random.normal(key_of[7], (D,), jnp.float32), 0.5, 1.5).astype(jnp.bfloat16),
        "w_in": normal_values(key_of[8], (D, 2 * FF), D ** -0.5, 0.15625, ((0, 8),)),
        "w_down": normal_values(key_of[9], (FF, D), FF ** -0.5, 0.09375, ((0, 8),)),
        "cotangent": normal_values(key_of[10], (TOKENS, D), 1.0, 6.0, ((0, 32),)),
    }


epsilon = 1e-06
masked = -1e+30

@jax.custom_vjp
def low(v):
    return lax.optimization_barrier(v.astype(jnp.bfloat16)).astype(jnp.float32)

@jax.custom_vjp
def low_back(v):
    return v

def low_keep(v):
    return (low(v), None)

def low_pass(kept, grad):
    return (grad,)

def back_keep(v):
    return (v, None)

def back_low(kept, grad):
    return (low(grad),)
low.defvjp(low_keep, low_pass)
low_back.defvjp(back_keep, back_low)

def product(left_side, right_side):
    return jnp.dot(left_side, right_side, precision=lax.Precision.HIGHEST, preferred_element_type=jnp.float32)

def rms_normed(values):
    return values * lax.rsqrt(lax.optimization_barrier(jnp.mean(values * values, axis=-1, keepdims=True)) + epsilon)

def shifted(values, mixing):
    earlier = jnp.concatenate([jnp.zeros_like(values[:1]), values[:-1]], axis=0)
    return (1.0 - mixing)[..., None] * values + mixing[..., None] * earlier

def attend_block(block_start, queries, key_rows, value_rows, totals):
    row_count = queries.shape[0]
    raw_dots = jnp.einsum('qhd,khd->hqk', queries, key_rows, precision=lax.Precision.HIGHEST) * HD ** (-0.5)
    raw_dots = low_back(raw_dots)
    row_totals = lax.dynamic_slice_in_dim(totals, block_start, row_count, 0)
    scores = raw_dots + row_totals.T[:, :, None] - totals.T[:, None, :]
    query_index = block_start + jnp.arange(row_count, dtype=jnp.int32)
    key_index = jnp.arange(key_rows.shape[0], dtype=jnp.int32)
    scores = jnp.where((key_index[None, :] <= query_index[:, None])[None], scores, masked)
    probabilities = low(jax.nn.softmax(scores, axis=-1))
    return jnp.einsum('hqk,khd->qhd', probabilities, value_rows, precision=lax.Precision.HIGHEST)

def residual_block(source, weight_list):
    norm_attn, w_proj, w_small, forget_bias, qk_gain, w_out, norm_ffn, w_in, w_down = weight_list
    length = source.shape[0]
    normed = low(rms_normed(source) * norm_attn)
    projected = low(low_back(product(normed, w_proj)))
    logits = low(low_back(product(normed, w_small)))
    query_raw = projected[:, :D].reshape(length, H, HD)
    key_raw = projected[:, D:2 * D].reshape(length, H, HD)
    value_raw = projected[:, 2 * D:3 * D].reshape(length, H, HD)
    out_gate = projected[:, 3 * D:]
    queries = low(rms_normed(query_raw) * qk_gain[0])
    key_mix = jax.nn.sigmoid(logits[:, H:2 * H])
    value_mix = jax.nn.sigmoid(logits[:, 2 * H:])
    key_rows = low(shifted(rms_normed(key_raw) * qk_gain[1], key_mix))
    value_rows = low(shifted(value_raw, value_mix))
    totals = jnp.cumsum(jax.nn.log_sigmoid(logits[:, :H] + forget_bias), axis=0)
    blocks = length // QBLOCK
    starts = jnp.arange(blocks, dtype=jnp.int32) * QBLOCK
    runner = jax.checkpoint(lambda head_item: attend_block(head_item[0], head_item[1], key_rows, value_rows, totals))
    attended = lax.map(runner, (starts, queries.reshape(blocks, QBLOCK, H, HD)))
    attended = low(low_back(attended.reshape(length, D)))
    gated_out = low(low_back(attended * jax.nn.sigmoid(out_gate)))
    residual = source + low_back(product(gated_out, w_out))
    normed_ffn = low(rms_normed(residual) * norm_ffn)
    gate_up = low_back(product(normed_ffn, w_in))
    activated = low(jax.nn.silu(gate_up[:, :FF]) * gate_up[:, FF:])
    return residual + product(activated, w_down)

def reference(inputs, norm_attn, w_proj, w_small, forget_bias, qk_gain, w_out, norm_ffn, w_in, w_down, cotangent):
    length = SEQ_ROWS * N_SEQ
    seq_count = inputs.shape[0] // length
    weight_list = tuple((tensor.astype(jnp.float32) for tensor in (norm_attn, w_proj, w_small, forget_bias, qk_gain, w_out, norm_ffn, w_in, w_down)))

    def whole_layer(source, weight_args):
        runner = jax.checkpoint(lambda sequence: residual_block(sequence, weight_args))
        return lax.map(runner, source.reshape(seq_count, length, D)).reshape(seq_count * length, D)
    output, pullback = jax.vjp(whole_layer, inputs.astype(jnp.float32), weight_list)
    grad_inputs, gradients = pullback(cotangent.astype(jnp.float32))
    return (output.astype(jnp.bfloat16), grad_inputs, gradients[0], gradients[1], gradients[2], gradients[3], gradients[4], gradients[5], gradients[6], gradients[7], gradients[8])
```

```python
from functools import partial

import jax
import jax.numpy as jnp
from jax import lax
from jax.experimental import pallas as pl
from jax.experimental.pallas import tpu as pltpu
from jax.sharding import PartitionSpec as P

epsilon = 1e-06
LANES = 128
QROWS = 256


def dot_ab(a, b):
    return lax.dot_general(a, b, (((1,), (0,)), ((), ())), preferred_element_type=jnp.float32)


def dot_abt(a, b):
    return lax.dot_general(a, b, (((1,), (1,)), ((), ())), preferred_element_type=jnp.float32)


def dot_atb(a, b):
    return lax.dot_general(a, b, (((0,), (0,)), ((), ())), preferred_element_type=jnp.float32)


def lane_ids(rows):
    return lax.broadcasted_iota(jnp.int32, (rows, LANES), 1)


def row_ids(rows):
    return lax.broadcasted_iota(jnp.int32, (rows, LANES), 0)


def group_sum(values, block_ones):
    high = values.astype(jnp.bfloat16)
    low = (values - high.astype(jnp.float32)).astype(jnp.bfloat16)
    return dot_ab(high, block_ones) + dot_ab(low, block_ones)


def selector(first_column, half):
    column = lax.broadcasted_iota(jnp.int32, (LANES, LANES), 0)
    lane = lax.broadcasted_iota(jnp.int32, (LANES, LANES), 1)
    wanted = first_column + (lane >= half).astype(jnp.int32)
    return (column == wanted).astype(jnp.float32).astype(jnp.bfloat16)


def prepare(q_ref, k_ref, v_ref, small_ref, bias_ref, gain_ref, heads):
    length = q_ref.shape[0]
    half = LANES // 2
    pair = pl.program_id(0)
    row_block = lax.broadcasted_iota(jnp.int32, (LANES, LANES), 0) >= half
    lane_block = lax.broadcasted_iota(jnp.int32, (LANES, LANES), 1) >= half
    block_ones = (row_block == lane_block).astype(jnp.float32).astype(jnp.bfloat16)
    first_row = row_ids(length) == 0
    query = q_ref[...].astype(jnp.float32)
    key = k_ref[...].astype(jnp.float32)
    value = v_ref[...].astype(jnp.float32)
    small = small_ref[...]
    factor_query = lax.rsqrt(group_sum(query * query, block_ones) * (1.0 / half) + epsilon)
    factor_key = lax.rsqrt(group_sum(key * key, block_ones) * (1.0 / half) + epsilon)
    unit_query = query * factor_query
    unit_key = key * factor_key
    key_normed = unit_key * gain_ref[1:2, :]
    forget = dot_ab(small, selector(2 * pair, half)) + bias_ref[0]
    key_mix = jax.nn.sigmoid(dot_ab(small, selector(heads + 2 * pair, half)))
    value_mix = jax.nn.sigmoid(dot_ab(small, selector(2 * heads + 2 * pair, half)))
    key_earlier = jnp.where(first_row, 0.0, pltpu.roll(key_normed, 1, 0))
    value_earlier = jnp.where(first_row, 0.0, pltpu.roll(value, 1, 0))
    queries = (unit_query * gain_ref[0:1, :]).astype(jnp.bfloat16)
    keys = ((1.0 - key_mix) * key_normed + key_mix * key_earlier).astype(jnp.bfloat16)
    values = ((1.0 - value_mix) * value + value_mix * value_earlier).astype(jnp.bfloat16)
    return dict(
        block_ones=block_ones, query=query, key=key, value=value, factor_query=factor_query,
        factor_key=factor_key, unit_query=unit_query, unit_key=unit_key, key_normed=key_normed,
        forget=forget, key_mix=key_mix, value_mix=value_mix, key_earlier=key_earlier,
        value_earlier=value_earlier, queries=queries, keys=keys, values=values,
    )


def running_sum(values, direction):
    length = values.shape[0]
    rows = row_ids(length)
    step = 1
    while step < length:
        if direction > 0:
            moved = jnp.where(rows >= step, pltpu.roll(values, step, 0), 0.0)
        else:
            moved = jnp.where(rows < length - step, pltpu.roll(values, length - step, 0), 0.0)
        values = values + moved
        step *= 2
    return values


def masked_head(values, head):
    lane = lane_ids(values.shape[0])
    keep = (lane < LANES // 2) if head == 0 else (lane >= LANES // 2)
    return jnp.where(keep, values, jnp.zeros_like(values))


def causal(scores, width, rows):
    diagonal = scores[:, width - rows :]
    query_index = lax.broadcasted_iota(jnp.int32, (rows, rows), 0)
    key_index = lax.broadcasted_iota(jnp.int32, (rows, rows), 1)
    diagonal = jnp.where(key_index <= query_index, diagonal, -1e30)
    if width == rows:
        return diagonal
    return jnp.concatenate([scores[:, : width - rows], diagonal], axis=1)


def attend_kernel(q_ref, k_ref, v_ref, g_ref, small_ref, bias_ref, gain_ref,
                  gated_ref, attended_ref, shift_ref, heads):
    length = q_ref.shape[0]
    half = LANES // 2
    p = prepare(q_ref, k_ref, v_ref, small_ref, bias_ref, gain_ref, heads)
    x = p["forget"]
    totals = running_sum(jnp.minimum(x, 0.0) - jnp.log1p(jnp.exp(-jnp.abs(x))), 1)
    totals_rows = totals.T
    scaled = p["queries"] * jnp.bfloat16(half ** -0.5)
    rows = min(QROWS, length)
    for start in range(0, length, rows):
        width = start + rows
        outs, shifts = [], []
        for head in range(2):
            query = masked_head(scaled[start:width], head)
            row_total = totals[start:width, head * half : head * half + 1]
            key_total = totals_rows[head * half : head * half + 1, :width]
            scores = dot_abt(query, p["keys"][:width]) + (row_total - key_total)
            exponent = jnp.exp(causal(scores, width, rows))
            row_sum = jnp.sum(exponent, axis=1, keepdims=True)
            probability = (exponent * (1.0 / row_sum)).astype(jnp.bfloat16)
            outs.append(dot_ab(probability, p["values"][:width]))
            shifts.append(row_total - jnp.log(row_sum))
        first = lane_ids(rows) < half
        attended = jnp.where(first, outs[0], outs[1]).astype(jnp.bfloat16)
        shift_ref[start:width, :] = jnp.where(first, shifts[0], shifts[1])
        attended_ref[start:width, :] = attended
        gate = jax.nn.sigmoid(g_ref[start:width, :].astype(jnp.float32))
        gated_ref[start:width, :] = (attended.astype(jnp.float32) * gate).astype(jnp.bfloat16)


def attend_back_kernel(q_ref, k_ref, v_ref, g_ref, small_ref, bias_ref, gain_ref,
                       attended_ref, shift_ref, grad_ref,
                       out_ref, gains_ref, forget_ref,
                       dq_ref, dk_ref, dv_ref, sums_ref, heads):
    length = q_ref.shape[0]
    half = LANES // 2
    pair = pl.program_id(0)
    pairs = heads // 2
    p = prepare(q_ref, k_ref, v_ref, small_ref, bias_ref, gain_ref, heads)
    x = p["forget"]
    totals_rows = running_sum(jnp.minimum(x, 0.0) - jnp.log1p(jnp.exp(-jnp.abs(x))), 1).T
    scale = jnp.bfloat16(half ** -0.5)
    scaled = p["queries"] * scale
    scaled_keys = p["keys"] * scale
    gate = jax.nn.sigmoid(g_ref[...].astype(jnp.float32))
    grad_gated = grad_ref[...].astype(jnp.float32)
    grad_attended = (grad_gated * gate).astype(jnp.bfloat16)

    def put(kind, values):
        at = pl.multiple_of((kind * pairs + pair) * LANES, LANES)
        out_ref[:, pl.ds(at, LANES)] = values.astype(jnp.bfloat16)

    put(3, grad_gated * attended_ref[...].astype(jnp.float32) * gate * (1.0 - gate))
    dk_ref[...] = jnp.zeros_like(dk_ref)
    dv_ref[...] = jnp.zeros_like(dv_ref)
    sums_ref[...] = jnp.zeros_like(sums_ref)
    rows = min(QROWS, length)
    row_parts = []
    for start in range(0, length, rows):
        width = start + rows
        first = lane_ids(rows) < half
        first_wide = lane_ids(width) < half
        dqs, dks, dvs, row_sums = [], [], [], []
        for head in range(2):
            query = masked_head(scaled[start:width], head)
            grad = masked_head(grad_attended[start:width], head)
            key_total = totals_rows[head * half : head * half + 1, :width]
            scores = dot_abt(query, p["keys"][:width]) + (
                shift_ref[start:width, head * half : head * half + 1] - key_total
            )
            probability = jnp.exp(causal(scores, width, rows))
            weighted = probability * dot_abt(grad, p["values"][:width])
            inner = jnp.sum(weighted, axis=1, keepdims=True)
            grad_scores = weighted - probability * inner
            row_sums.append(jnp.sum(grad_scores, axis=1, keepdims=True))
            sums_ref[head : head + 1, :width] += jnp.sum(grad_scores, axis=0, keepdims=True)
            low = grad_scores.astype(jnp.bfloat16)
            dqs.append(dot_ab(low, scaled_keys[:width]))
            dks.append(dot_atb(low, scaled[start:width]))
            dvs.append(dot_atb(probability.astype(jnp.bfloat16), grad_attended[start:width]))
        dq_ref[start:width, :] = jnp.where(first, dqs[0], dqs[1])
        dk_ref[:width, :] += jnp.where(first_wide, dks[0], dks[1])
        dv_ref[:width, :] += jnp.where(first_wide, dvs[0], dvs[1])
        row_parts.append(jnp.where(first, row_sums[0], row_sums[1]))
    lane = lane_ids(length)
    top = lax.broadcasted_iota(jnp.int32, (LANES, length), 0) < half
    columns = jnp.where(top, sums_ref[0:1, :], sums_ref[1:2, :]).T
    grad_totals = jnp.concatenate(row_parts, axis=0) - columns
    grad_forget = running_sum(grad_totals, -1) * (1.0 - jax.nn.sigmoid(x))

    def unshift(grad, mixing, values, earlier):
        carried = mixing * grad
        following = jnp.where(row_ids(length) == length - 1, 0.0, pltpu.roll(carried, length - 1, 0))
        grad_mixing = group_sum(grad * (earlier - values), p["block_ones"])
        return (1.0 - mixing) * grad + following, grad_mixing * mixing * (1.0 - mixing)

    def norm_back(factor, unit, grad):
        inner = group_sum(grad * unit, p["block_ones"]) * (1.0 / half)
        return factor * (grad - unit * inner)

    grad_query = dq_ref[...]
    grad_key, grad_key_mix = unshift(dk_ref[...], p["key_mix"], p["key_normed"], p["key_earlier"])
    grad_value, grad_value_mix = unshift(dv_ref[...], p["value_mix"], p["value"], p["value_earlier"])
    put(0, norm_back(p["factor_query"], p["unit_query"], grad_query * gain_ref[0:1, :]))
    put(1, norm_back(p["factor_key"], p["unit_key"], grad_key * gain_ref[1:2, :]))
    put(2, grad_value)

    @pl.when(pair == 0)
    def _():
        out_ref[:, 4 * pairs * LANES :] = jnp.zeros((length, LANES), jnp.bfloat16)
        gains_ref[...] = jnp.zeros_like(gains_ref)

    gains_ref[0:1, :] += jnp.sum(grad_query * p["unit_query"], axis=0, keepdims=True)
    gains_ref[1:2, :] += jnp.sum(grad_key * p["unit_key"], axis=0, keepdims=True)
    forget_ref[0] = jnp.sum(grad_forget, axis=0, keepdims=True)
    merged = out_ref[:, 4 * pairs * LANES :].astype(jnp.float32)
    for kind, values in enumerate((grad_forget, grad_key_mix, grad_value_mix)):
        swapped = pltpu.roll(values, half, 1)
        first = jnp.where(lane < half, values, swapped)
        second = jnp.where(lane < half, swapped, values)
        column = kind * heads + 2 * pair
        merged = jnp.where(lane == column, first, jnp.where(lane == column + 1, second, merged))
    out_ref[:, 4 * pairs * LANES :] = merged.astype(jnp.bfloat16)


def block_specs(length, pairs):
    def column(kind):
        return pl.BlockSpec((length, LANES), lambda i: (0, kind * pairs + i))

    return [
        column(0), column(1), column(2), column(3),
        pl.BlockSpec((length, LANES), lambda i: (0, 4 * pairs)),
        pl.BlockSpec((1, 1, LANES), lambda i: (i, 0, 0)),
        pl.BlockSpec((2, LANES), lambda i: (0, 0)),
    ]


def attend(projected, bias, gains, heads):
    length = projected.shape[0]
    pairs = heads // 2
    block = pl.BlockSpec((length, LANES), lambda i: (0, i))
    wide = pairs * LANES
    return pl.pallas_call(
        partial(attend_kernel, heads=heads),
        grid=(pairs,),
        in_specs=block_specs(length, pairs),
        out_specs=[block, block, block],
        out_shape=[
            jax.ShapeDtypeStruct((length, wide), jnp.bfloat16),
            jax.ShapeDtypeStruct((length, wide), jnp.bfloat16),
            jax.ShapeDtypeStruct((length, wide), jnp.float32),
        ],
        compiler_params=pltpu.CompilerParams(vmem_limit_bytes=48 * 2**20),
        cost_estimate=pl.CostEstimate(
            flops=2 * 2 * length * length * wide, transcendentals=length * length * heads // 2,
            bytes_accessed=length * wide * 2 * 10,
        ),
        name="attend",
    )(projected, projected, projected, projected, projected, bias, gains)


def attend_back(projected, bias, gains, attended, shift, grad, heads):
    length, full = projected.shape
    pairs = heads // 2
    wide = pairs * LANES
    block = pl.BlockSpec((length, LANES), lambda i: (0, i))
    return pl.pallas_call(
        partial(attend_back_kernel, heads=heads),
        grid=(pairs,),
        in_specs=block_specs(length, pairs) + [block, block, block],
        out_specs=[
            pl.BlockSpec((length, full), lambda i: (0, 0)),
            pl.BlockSpec((2, LANES), lambda i: (0, 0)),
            pl.BlockSpec((1, 1, LANES), lambda i: (i, 0, 0)),
        ],
        out_shape=[
            jax.ShapeDtypeStruct((length, full), jnp.bfloat16),
            jax.ShapeDtypeStruct((2, LANES), jnp.float32),
            jax.ShapeDtypeStruct((pairs, 1, LANES), jnp.float32),
        ],
        scratch_shapes=[
            pltpu.VMEM((length, LANES), jnp.float32),
            pltpu.VMEM((length, LANES), jnp.float32),
            pltpu.VMEM((length, LANES), jnp.float32),
            pltpu.VMEM((8, length), jnp.float32),
        ],
        compiler_params=pltpu.CompilerParams(vmem_limit_bytes=48 * 2**20),
        cost_estimate=pl.CostEstimate(
            flops=5 * 2 * length * length * wide, transcendentals=length * length * heads // 2,
            bytes_accessed=length * wide * 2 * 16,
        ),
        name="attend_back",
    )(projected, projected, projected, projected, projected, bias, gains, attended, shift, grad)


def inverse_norm(values):
    return lax.rsqrt(jnp.mean(values * values, axis=-1, keepdims=True) + epsilon)


def norm_back(values, factor, grad_normed):
    normed = values * factor
    inner_mean = jnp.mean(grad_normed * normed, axis=-1, keepdims=True)
    return factor * (grad_normed - normed * inner_mean)


def swap_with(values, axis, bit):
    size = lax.axis_size(axis)
    return lax.ppermute(values, axis, [(i, i ^ bit) for i in range(size)])


def line_gather(block, axis):
    size = lax.axis_size(axis)
    index = lax.axis_index(axis)
    rows = block.shape[0]
    rising, falling = [], []
    up = down = block
    for _ in range(size - 1):
        up = lax.ppermute(up, axis, [(i, i + 1) for i in range(size - 1)])
        down = lax.ppermute(down, axis, [(i + 1, i) for i in range(size - 1)])
        rising.append(up)
        falling.append(down)
    ordered = jnp.concatenate(rising[::-1] + [block] + falling, axis=0)
    return lax.dynamic_slice_in_dim(ordered, (size - 1 - index) * rows, size * rows, 0)


def line_scatter(partial_rows, axis):
    size = lax.axis_size(axis)
    index = lax.axis_index(axis)
    rows = partial_rows.shape[0] // size

    def part(at):
        return lax.dynamic_slice_in_dim(partial_rows, jnp.clip(at, 0, size - 1) * rows, rows, 0)

    up = down = None
    for step in range(1, size):
        far = size - step
        above, below = part(index + far), part(index - far)
        if up is not None:
            above, below = above + up, below + down
        up = lax.ppermute(
            above.astype(jnp.bfloat16), axis, [(i, i + 1) for i in range(size - 1)]
        ).astype(jnp.float32)
        down = lax.ppermute(
            below.astype(jnp.bfloat16), axis, [(i + 1, i) for i in range(size - 1)]
        ).astype(jnp.float32)
    return part(index) + up + down


def sum_everywhere(values, axes):
    for axis in axes:
        bit = 1
        while bit < lax.axis_size(axis):
            values = values + swap_with(values, axis, bit)
            bit *= 2
    return values


def body(
    inputs,
    norm_attn,
    w_proj,
    w_small,
    forget_bias,
    qk_gain,
    w_out,
    norm_ffn,
    w_in,
    w_down,
    cotangent,
):
    row_count, model_width = inputs.shape
    weight_rows = w_proj.shape[0]
    seq_parts = lax.axis_size("seq")
    fsdp_parts = lax.axis_size("fsdp")
    seq_at = lax.axis_index("seq")
    side = seq_at % 2
    head_count = forget_bias.shape[0]
    head_width = qk_gain.shape[1]
    heads = head_count // seq_parts
    wide = heads * head_width
    small_wide = 3 * heads
    length = row_count * seq_parts
    hidden_rows = w_down.shape[0]
    hidden_half = fsdp_parts * hidden_rows // 2

    every_input = line_gather(inputs, "seq")
    local_proj = lax.dynamic_index_in_dim(
        w_proj.reshape(weight_rows, 4, seq_parts, wide), seq_at, 2, False
    ).reshape(weight_rows, 4 * wide)
    local_small = lax.dynamic_index_in_dim(
        w_small.reshape(weight_rows, 3, seq_parts, heads), seq_at, 2, False
    ).reshape(weight_rows, small_wide)
    packed = jnp.concatenate(
        [
            local_proj,
            local_small,
            norm_attn[:, None],
            norm_ffn[:, None],
            jnp.zeros((weight_rows, LANES - small_wide - 2), jnp.bfloat16),
        ],
        axis=1,
    )
    packed_full = lax.all_gather(packed, "fsdp", axis=0, tiled=True)
    gain_attention = packed_full[:, 4 * wide + small_wide].astype(jnp.float32)
    gain_ffn = packed_full[:, 4 * wide + small_wide + 1].astype(jnp.float32)
    out_full = lax.all_gather(w_out, "fsdp", axis=0, tiled=True)
    in_half = lax.dynamic_index_in_dim(
        w_in.reshape(weight_rows, 2, fsdp_parts, 2, hidden_rows // 2), side, 3, False
    ).reshape(weight_rows, 2 * hidden_half)
    in_half = lax.all_gather(in_half, "fsdp", axis=0, tiled=True)
    down_half = lax.dynamic_index_in_dim(
        w_down.reshape(2, hidden_rows // 2, model_width), side, 0, False
    )
    down_half = lax.all_gather(down_half, "fsdp", axis=0, tiled=True)
    cotangent_pair = jnp.concatenate([cotangent, swap_with(cotangent, "seq", 1)], axis=0)

    wide_input = every_input.astype(jnp.float32)
    normed = (wide_input * inverse_norm(wide_input) * gain_attention).astype(jnp.bfloat16)
    projected = dot_ab(normed, packed_full).astype(jnp.bfloat16)
    bias_lanes = jnp.repeat(
        lax.dynamic_slice_in_dim(forget_bias, seq_at * heads, heads, 0), head_width
    ).reshape(heads // 2, 1, LANES)
    gain_lanes = jnp.tile(qk_gain.astype(jnp.float32), (1, 2))
    gated, attended, shift = attend(projected, bias_lanes, gain_lanes, heads)
    mixed_rows = lax.all_to_all(gated, "seq", split_axis=0, concat_axis=1, tiled=True)

    source = inputs.astype(jnp.float32)
    residual = source + dot_ab(mixed_rows, out_full)
    factor_ffn = inverse_norm(residual)
    unit_ffn = residual * factor_ffn
    normed_ffn = (unit_ffn * gain_ffn).astype(jnp.bfloat16)
    normed_pair = jnp.concatenate([normed_ffn, swap_with(normed_ffn, "seq", 1)], axis=0)
    gate_up = dot_ab(normed_pair, in_half)
    gate_part = gate_up[:, :hidden_half]
    up_part = gate_up[:, hidden_half:]
    inner_sigmoid = jax.nn.sigmoid(gate_part)
    silu_gate = gate_part * inner_sigmoid
    activated = (silu_gate * up_part).astype(jnp.bfloat16)
    down_part = dot_ab(activated, down_half)
    output = (
        residual
        + down_part[:row_count]
        + swap_with(down_part[row_count:].astype(jnp.bfloat16), "seq", 1).astype(jnp.float32)
    ).astype(jnp.bfloat16)

    grad_act = dot_abt(cotangent_pair, down_half)
    grad_gate = grad_act * up_part * inner_sigmoid * (1.0 + gate_part * (1.0 - inner_sigmoid))
    grad_up = grad_act * silu_gate
    grad_gate_up = jnp.concatenate([grad_gate, grad_up], axis=1).astype(jnp.bfloat16)
    back_part = dot_abt(grad_gate_up, in_half)
    grad_normed_ffn = back_part[:row_count] + swap_with(
        back_part[row_count:].astype(jnp.bfloat16), "seq", 1
    ).astype(jnp.float32)
    grad_residual = cotangent.astype(jnp.float32) + norm_back(
        residual, factor_ffn, grad_normed_ffn * gain_ffn
    )
    grad_branch = grad_residual.astype(jnp.bfloat16)
    grad_mixed = dot_abt(grad_branch, out_full).astype(jnp.bfloat16)
    grad_heads = lax.all_to_all(grad_mixed, "seq", split_axis=1, concat_axis=0, tiled=True)
    grad_down = dot_atb(activated, cotangent_pair).astype(jnp.bfloat16)
    grad_in = dot_atb(normed_pair, grad_gate_up).astype(jnp.bfloat16)
    grad_out = dot_atb(mixed_rows, grad_branch).astype(jnp.bfloat16)
    grad_in = lax.psum_scatter(grad_in, "fsdp", scatter_dimension=0, tiled=True)
    grad_down = lax.psum_scatter(grad_down, "fsdp", scatter_dimension=0, tiled=True)
    grad_out = lax.psum_scatter(grad_out, "fsdp", scatter_dimension=0, tiled=True)

    grad_projected, gain_sums, forget_sums = attend_back(
        projected, bias_lanes, gain_lanes, attended, shift, grad_heads, heads
    )
    grad_packed = dot_atb(normed, grad_projected).astype(jnp.bfloat16)
    grad_packed = lax.psum_scatter(grad_packed, "fsdp", scatter_dimension=0, tiled=True)
    grad_normed = line_scatter(dot_abt(grad_projected, packed_full), "seq")
    grad_inputs = grad_residual + norm_back(
        source, inverse_norm(source), grad_normed * gain_attention
    )

    bias_row = lax.dynamic_update_slice_in_dim(
        jnp.zeros((LANES,), jnp.float32),
        forget_sums.reshape(heads, head_width)[:, 0],
        seq_at * heads,
        0,
    )
    sums = sum_everywhere(jnp.concatenate([gain_sums, bias_row[None]], axis=0), ("fsdp", "seq"))
    grad_qk_gain = sums[:2, :head_width] + sums[:2, head_width:]
    grad_forget_bias = sums[2, :head_count]

    def whole_hidden(half):
        total = half.astype(jnp.float32)
        bit = 2
        while bit < seq_parts:
            moved = swap_with(total.astype(jnp.bfloat16), "seq", bit).astype(jnp.float32)
            total = total + moved
            bit *= 2
        total = total.astype(jnp.bfloat16)
        other = swap_with(total, "seq", 1)
        first = jnp.where(side == 0, total, other)
        second = jnp.where(side == 0, other, total)
        return first.astype(jnp.float32), second.astype(jnp.float32)

    first, second = whole_hidden(grad_in)
    folded = (weight_rows, 2, fsdp_parts, 1, hidden_rows // 2)
    grad_in = jnp.concatenate([first.reshape(folded), second.reshape(folded)], axis=3).reshape(
        weight_rows, 4 * hidden_half
    )
    grad_down = jnp.concatenate(whole_hidden(grad_down), axis=0)
    grad_out = lax.psum(grad_out, "seq").astype(jnp.float32)
    every_packed = lax.all_gather(grad_packed, "seq", axis=0, tiled=False).astype(jnp.float32)
    grad_proj = jnp.moveaxis(
        every_packed[:, :, : 4 * wide].reshape(seq_parts, weight_rows, 4, wide), 0, 2
    ).reshape(weight_rows, 4 * seq_parts * wide)
    grad_small = jnp.moveaxis(
        every_packed[:, :, 4 * wide : 4 * wide + small_wide].reshape(
            seq_parts, weight_rows, 3, heads
        ),
        0,
        2,
    ).reshape(weight_rows, 3 * head_count)
    grad_gain_attention = (
        jnp.sum(grad_proj * w_proj.astype(jnp.float32), axis=1)
        + jnp.sum(grad_small * w_small.astype(jnp.float32), axis=1)
    ) / norm_attn.astype(jnp.float32)
    grad_gain_ffn = jnp.sum(grad_in * w_in.astype(jnp.float32), axis=1) / norm_ffn.astype(
        jnp.float32
    )
    return (
        output,
        grad_inputs,
        grad_gain_attention,
        grad_proj,
        grad_small,
        grad_forget_bias,
        grad_qk_gain,
        grad_out,
        grad_gain_ffn,
        grad_in,
        grad_down,
    )


def solution(mesh):
    in_specs = (
        P(("fsdp", "seq"), None),
        P("fsdp"),
        P("fsdp", None),
        P("fsdp", None),
        P(),
        P(),
        P("fsdp", None),
        P("fsdp"),
        P("fsdp", None),
        P("fsdp", None),
        P(("fsdp", "seq"), None),
    )
    out_specs = (
        P(("fsdp", "seq"), None),
        P(("fsdp", "seq"), None),
        P("fsdp"),
        P("fsdp", None),
        P("fsdp", None),
        P(),
        P(),
        P("fsdp", None),
        P("fsdp"),
        P("fsdp", None),
        P("fsdp", None),
    )
    return jax.shard_map(body, mesh=mesh, in_specs=in_specs, out_specs=out_specs, check_vma=False)
```

```python
from functools import partial

import jax
import jax.numpy as jnp
from jax import lax
from jax.experimental import pallas as pl
from jax.experimental.pallas import tpu as pltpu
from jax.sharding import PartitionSpec as P

epsilon = 1e-06
LANES = 128
QROWS = 256


def dot_ab(a, b):
    return lax.dot_general(a, b, (((1,), (0,)), ((), ())), preferred_element_type=jnp.float32)


def dot_abt(a, b):
    return lax.dot_general(a, b, (((1,), (1,)), ((), ())), preferred_element_type=jnp.float32)


def dot_atb(a, b):
    return lax.dot_general(a, b, (((0,), (0,)), ((), ())), preferred_element_type=jnp.float32)


def lane_ids(rows):
    return lax.broadcasted_iota(jnp.int32, (rows, LANES), 1)


def row_ids(rows):
    return lax.broadcasted_iota(jnp.int32, (rows, LANES), 0)


def group_sum(values, block_ones):
    high = values.astype(jnp.bfloat16)
    low = (values - high.astype(jnp.float32)).astype(jnp.bfloat16)
    return dot_ab(high, block_ones) + dot_ab(low, block_ones)


def selector(first_column, half):
    column = lax.broadcasted_iota(jnp.int32, (LANES, LANES), 0)
    lane = lax.broadcasted_iota(jnp.int32, (LANES, LANES), 1)
    wanted = first_column + (lane >= half).astype(jnp.int32)
    return (column == wanted).astype(jnp.float32).astype(jnp.bfloat16)


def prepare(q_ref, k_ref, v_ref, small_ref, bias_ref, gain_ref, heads):
    length = q_ref.shape[0]
    half = LANES // 2
    pair = pl.program_id(0)
    row_block = lax.broadcasted_iota(jnp.int32, (LANES, LANES), 0) >= half
    lane_block = lax.broadcasted_iota(jnp.int32, (LANES, LANES), 1) >= half
    block_ones = (row_block == lane_block).astype(jnp.float32).astype(jnp.bfloat16)
    first_row = row_ids(length) == 0
    query = q_ref[...].astype(jnp.float32)
    key = k_ref[...].astype(jnp.float32)
    value = v_ref[...].astype(jnp.float32)
    small = small_ref[...]
    factor_query = lax.rsqrt(group_sum(query * query, block_ones) * (1.0 / half) + epsilon)
    factor_key = lax.rsqrt(group_sum(key * key, block_ones) * (1.0 / half) + epsilon)
    unit_query = query * factor_query
    unit_key = key * factor_key
    key_normed = unit_key * gain_ref[1:2, :]
    forget = dot_ab(small, selector(2 * pair, half)) + bias_ref[0]
    key_mix = jax.nn.sigmoid(dot_ab(small, selector(heads + 2 * pair, half)))
    value_mix = jax.nn.sigmoid(dot_ab(small, selector(2 * heads + 2 * pair, half)))
    key_earlier = jnp.where(first_row, 0.0, pltpu.roll(key_normed, 1, 0))
    value_earlier = jnp.where(first_row, 0.0, pltpu.roll(value, 1, 0))
    queries = (unit_query * gain_ref[0:1, :]).astype(jnp.bfloat16)
    keys = ((1.0 - key_mix) * key_normed + key_mix * key_earlier).astype(jnp.bfloat16)
    values = ((1.0 - value_mix) * value + value_mix * value_earlier).astype(jnp.bfloat16)
    return dict(
        block_ones=block_ones, query=query, key=key, value=value, factor_query=factor_query,
        factor_key=factor_key, unit_query=unit_query, unit_key=unit_key, key_normed=key_normed,
        forget=forget, key_mix=key_mix, value_mix=value_mix, key_earlier=key_earlier,
        value_earlier=value_earlier, queries=queries, keys=keys, values=values,
    )


def running_sum(values, direction):
    length = values.shape[0]
    rows = row_ids(length)
    step = 1
    while step < length:
        if direction > 0:
            moved = jnp.where(rows >= step, pltpu.roll(values, step, 0), 0.0)
        else:
            moved = jnp.where(rows < length - step, pltpu.roll(values, length - step, 0), 0.0)
        values = values + moved
        step *= 2
    return values


def masked_head(values, head):
    lane = lane_ids(values.shape[0])
    keep = (lane < LANES // 2) if head == 0 else (lane >= LANES // 2)
    return jnp.where(keep, values, jnp.zeros_like(values))


def causal(scores, width, rows):
    diagonal = scores[:, width - rows :]
    query_index = lax.broadcasted_iota(jnp.int32, (rows, rows), 0)
    key_index = lax.broadcasted_iota(jnp.int32, (rows, rows), 1)
    diagonal = jnp.where(key_index <= query_index, diagonal, -1e30)
    if width == rows:
        return diagonal
    return jnp.concatenate([scores[:, : width - rows], diagonal], axis=1)


def attend_kernel(q_ref, k_ref, v_ref, g_ref, small_ref, bias_ref, gain_ref,
                  gated_ref, attended_ref, shift_ref, heads):
    length = q_ref.shape[0]
    half = LANES // 2
    p = prepare(q_ref, k_ref, v_ref, small_ref, bias_ref, gain_ref, heads)
    x = p["forget"]
    totals = running_sum(jnp.minimum(x, 0.0) - jnp.log1p(jnp.exp(-jnp.abs(x))), 1)
    totals_rows = totals.T
    scaled = p["queries"] * jnp.bfloat16(half ** -0.5)
    rows = min(QROWS, length)
    for start in range(0, length, rows):
        width = start + rows
        outs, shifts = [], []
        for head in range(2):
            query = masked_head(scaled[start:width], head)
            row_total = totals[start:width, head * half : head * half + 1]
            key_total = totals_rows[head * half : head * half + 1, :width]
            scores = dot_abt(query, p["keys"][:width]) + (row_total - key_total)
            exponent = jnp.exp(causal(scores, width, rows))
            row_sum = jnp.sum(exponent, axis=1, keepdims=True)
            probability = (exponent * (1.0 / row_sum)).astype(jnp.bfloat16)
            outs.append(dot_ab(probability, p["values"][:width]))
            shifts.append(row_total - jnp.log(row_sum))
        first = lane_ids(rows) < half
        attended = jnp.where(first, outs[0], outs[1]).astype(jnp.bfloat16)
        shift_ref[start:width, :] = jnp.where(first, shifts[0], shifts[1])
        attended_ref[start:width, :] = attended
        gate = jax.nn.sigmoid(g_ref[start:width, :].astype(jnp.float32))
        gated_ref[start:width, :] = (attended.astype(jnp.float32) * gate).astype(jnp.bfloat16)


def attend_back_kernel(q_ref, k_ref, v_ref, g_ref, small_ref, bias_ref, gain_ref,
                       attended_ref, shift_ref, grad_ref,
                       out_ref, gains_ref, forget_ref,
                       dq_ref, dk_ref, dv_ref, sums_ref, heads):
    length = q_ref.shape[0]
    half = LANES // 2
    pair = pl.program_id(0)
    pairs = heads // 2
    p = prepare(q_ref, k_ref, v_ref, small_ref, bias_ref, gain_ref, heads)
    x = p["forget"]
    totals_rows = running_sum(jnp.minimum(x, 0.0) - jnp.log1p(jnp.exp(-jnp.abs(x))), 1).T
    scale = jnp.bfloat16(half ** -0.5)
    scaled = p["queries"] * scale
    scaled_keys = p["keys"] * scale
    gate = jax.nn.sigmoid(g_ref[...].astype(jnp.float32))
    grad_gated = grad_ref[...].astype(jnp.float32)
    grad_attended = (grad_gated * gate).astype(jnp.bfloat16)

    def put(kind, values):
        at = pl.multiple_of((kind * pairs + pair) * LANES, LANES)
        out_ref[:, pl.ds(at, LANES)] = values.astype(jnp.bfloat16)

    put(3, grad_gated * attended_ref[...].astype(jnp.float32) * gate * (1.0 - gate))
    dk_ref[...] = jnp.zeros_like(dk_ref)
    dv_ref[...] = jnp.zeros_like(dv_ref)
    sums_ref[...] = jnp.zeros_like(sums_ref)
    rows = min(QROWS, length)
    row_parts = []
    for start in range(0, length, rows):
        width = start + rows
        first = lane_ids(rows) < half
        first_wide = lane_ids(width) < half
        dqs, dks, dvs, row_sums = [], [], [], []
        for head in range(2):
            query = masked_head(scaled[start:width], head)
            grad = masked_head(grad_attended[start:width], head)
            key_total = totals_rows[head * half : head * half + 1, :width]
            scores = dot_abt(query, p["keys"][:width]) + (
                shift_ref[start:width, head * half : head * half + 1] - key_total
            )
            probability = jnp.exp(causal(scores, width, rows))
            weighted = probability * dot_abt(grad, p["values"][:width])
            inner = jnp.sum(weighted, axis=1, keepdims=True)
            grad_scores = weighted - probability * inner
            row_sums.append(jnp.sum(grad_scores, axis=1, keepdims=True))
            sums_ref[head : head + 1, :width] += jnp.sum(grad_scores, axis=0, keepdims=True)
            low = grad_scores.astype(jnp.bfloat16)
            dqs.append(dot_ab(low, scaled_keys[:width]))
            dks.append(dot_atb(low, scaled[start:width]))
            dvs.append(dot_atb(probability.astype(jnp.bfloat16), grad_attended[start:width]))
        dq_ref[start:width, :] = jnp.where(first, dqs[0], dqs[1])
        dk_ref[:width, :] += jnp.where(first_wide, dks[0], dks[1])
        dv_ref[:width, :] += jnp.where(first_wide, dvs[0], dvs[1])
        row_parts.append(jnp.where(first, row_sums[0], row_sums[1]))
    lane = lane_ids(length)
    top = lax.broadcasted_iota(jnp.int32, (LANES, length), 0) < half
    columns = jnp.where(top, sums_ref[0:1, :], sums_ref[1:2, :]).T
    grad_totals = jnp.concatenate(row_parts, axis=0) - columns
    grad_forget = running_sum(grad_totals, -1) * (1.0 - jax.nn.sigmoid(x))

    def unshift(grad, mixing, values, earlier):
        carried = mixing * grad
        following = jnp.where(row_ids(length) == length - 1, 0.0, pltpu.roll(carried, length - 1, 0))
        grad_mixing = group_sum(grad * (earlier - values), p["block_ones"])
        return (1.0 - mixing) * grad + following, grad_mixing * mixing * (1.0 - mixing)

    def norm_back(factor, unit, grad):
        inner = group_sum(grad * unit, p["block_ones"]) * (1.0 / half)
        return factor * (grad - unit * inner)

    grad_query = dq_ref[...]
    grad_key, grad_key_mix = unshift(dk_ref[...], p["key_mix"], p["key_normed"], p["key_earlier"])
    grad_value, grad_value_mix = unshift(dv_ref[...], p["value_mix"], p["value"], p["value_earlier"])
    put(0, norm_back(p["factor_query"], p["unit_query"], grad_query * gain_ref[0:1, :]))
    put(1, norm_back(p["factor_key"], p["unit_key"], grad_key * gain_ref[1:2, :]))
    put(2, grad_value)

    @pl.when(pair == 0)
    def _():
        out_ref[:, 4 * pairs * LANES :] = jnp.zeros((length, LANES), jnp.bfloat16)
        gains_ref[...] = jnp.zeros_like(gains_ref)

    gains_ref[0:1, :] += jnp.sum(grad_query * p["unit_query"], axis=0, keepdims=True)
    gains_ref[1:2, :] += jnp.sum(grad_key * p["unit_key"], axis=0, keepdims=True)
    forget_ref[0] = jnp.sum(grad_forget, axis=0, keepdims=True)
    merged = out_ref[:, 4 * pairs * LANES :].astype(jnp.float32)
    for kind, values in enumerate((grad_forget, grad_key_mix, grad_value_mix)):
        swapped = pltpu.roll(values, half, 1)
        first = jnp.where(lane < half, values, swapped)
        second = jnp.where(lane < half, swapped, values)
        column = kind * heads + 2 * pair
        merged = jnp.where(lane == column, first, jnp.where(lane == column + 1, second, merged))
    out_ref[:, 4 * pairs * LANES :] = merged.astype(jnp.bfloat16)


def block_specs(length, pairs):
    def column(kind):
        return pl.BlockSpec((length, LANES), lambda i: (0, kind * pairs + i))

    return [
        column(0), column(1), column(2), column(3),
        pl.BlockSpec((length, LANES), lambda i: (0, 4 * pairs)),
        pl.BlockSpec((1, 1, LANES), lambda i: (i, 0, 0)),
        pl.BlockSpec((2, LANES), lambda i: (0, 0)),
    ]


def attend(projected, bias, gains, heads):
    length = projected.shape[0]
    pairs = heads // 2
    block = pl.BlockSpec((length, LANES), lambda i: (0, i))
    wide = pairs * LANES
    return pl.pallas_call(
        partial(attend_kernel, heads=heads),
        grid=(pairs,),
        in_specs=block_specs(length, pairs),
        out_specs=[block, block, block],
        out_shape=[
            jax.ShapeDtypeStruct((length, wide), jnp.bfloat16),
            jax.ShapeDtypeStruct((length, wide), jnp.bfloat16),
            jax.ShapeDtypeStruct((length, wide), jnp.float32),
        ],
        compiler_params=pltpu.CompilerParams(vmem_limit_bytes=48 * 2**20),
        cost_estimate=pl.CostEstimate(
            flops=2 * 2 * length * length * wide, transcendentals=length * length * heads // 2,
            bytes_accessed=length * wide * 2 * 10,
        ),
        name="attend",
    )(projected, projected, projected, projected, projected, bias, gains)


def attend_back(projected, bias, gains, attended, shift, grad, heads):
    length, full = projected.shape
    pairs = heads // 2
    wide = pairs * LANES
    block = pl.BlockSpec((length, LANES), lambda i: (0, i))
    return pl.pallas_call(
        partial(attend_back_kernel, heads=heads),
        grid=(pairs,),
        in_specs=block_specs(length, pairs) + [block, block, block],
        out_specs=[
            pl.BlockSpec((length, full), lambda i: (0, 0)),
            pl.BlockSpec((2, LANES), lambda i: (0, 0)),
            pl.BlockSpec((1, 1, LANES), lambda i: (i, 0, 0)),
        ],
        out_shape=[
            jax.ShapeDtypeStruct((length, full), jnp.bfloat16),
            jax.ShapeDtypeStruct((2, LANES), jnp.float32),
            jax.ShapeDtypeStruct((pairs, 1, LANES), jnp.float32),
        ],
        scratch_shapes=[
            pltpu.VMEM((length, LANES), jnp.float32),
            pltpu.VMEM((length, LANES), jnp.float32),
            pltpu.VMEM((length, LANES), jnp.float32),
            pltpu.VMEM((8, length), jnp.float32),
        ],
        compiler_params=pltpu.CompilerParams(vmem_limit_bytes=48 * 2**20),
        cost_estimate=pl.CostEstimate(
            flops=5 * 2 * length * length * wide, transcendentals=length * length * heads // 2,
            bytes_accessed=length * wide * 2 * 16,
        ),
        name="attend_back",
    )(projected, projected, projected, projected, projected, bias, gains, attended, shift, grad)


def pack_kernel(at_ref, proj_ref, tail_ref, in_ref, packed_ref, own_ref, send_ref, sems,
                seq_parts, wide, blocks):
    seq_at, own, send = at_ref[0], at_ref[1], at_ref[2]
    copies = []

    def copy(source, target):
        copies.append(pltpu.make_async_copy(source, target, sems.at[len(copies)]))

    for kind in range(4):
        at = pl.multiple_of(kind * seq_parts * wide + seq_at * wide, LANES)
        copy(proj_ref.at[:, pl.ds(at, wide)], packed_ref.at[:, pl.ds(kind * wide, wide)])
    copy(tail_ref, packed_ref.at[:, pl.ds(4 * wide, LANES)])
    for block in range(blocks):
        for target, quarter in ((own_ref, own), (send_ref, send)):
            at = pl.multiple_of((block * 4 + quarter) * LANES, LANES)
            copy(in_ref.at[:, pl.ds(at, LANES)], target.at[:, pl.ds(block * LANES, LANES)])
    for item in copies:
        item.start()
    for item in copies:
        item.wait()


def pack(w_proj, tail, w_in, seq_at, own, send, seq_parts, quarter_rows):
    rows, hidden = w_in.shape[0], w_in.shape[1]
    wide = w_proj.shape[1] // 4 // seq_parts
    if quarter_rows % LANES:
        local = lax.dynamic_index_in_dim(
            w_proj.reshape(rows, 4, seq_parts, wide), seq_at, 2, False
        ).reshape(rows, 4 * wide)
        folded = w_in.reshape(rows, -1, 4, quarter_rows)
        return (
            jnp.concatenate([local, tail], axis=1),
            lax.dynamic_index_in_dim(folded, own, 2, False).reshape(rows, hidden // 4),
            lax.dynamic_index_in_dim(folded, send, 2, False).reshape(rows, hidden // 4),
        )
    blocks = hidden // 4 // LANES
    anywhere = pl.BlockSpec(memory_space=pl.ANY)
    return pl.pallas_call(
        partial(pack_kernel, seq_parts=seq_parts, wide=wide, blocks=blocks),
        grid_spec=pltpu.PrefetchScalarGridSpec(
            num_scalar_prefetch=1,
            grid=(1,),
            in_specs=[anywhere] * 3,
            out_specs=[anywhere] * 3,
            scratch_shapes=[pltpu.SemaphoreType.DMA((5 + 2 * blocks,))],
        ),
        out_shape=[
            jax.ShapeDtypeStruct((rows, 4 * wide + LANES), jnp.bfloat16),
            jax.ShapeDtypeStruct((rows, hidden // 4), jnp.bfloat16),
            jax.ShapeDtypeStruct((rows, hidden // 4), jnp.bfloat16),
        ],
        compiler_params=pltpu.CompilerParams(vmem_limit_bytes=4 * 2**20),
        cost_estimate=pl.CostEstimate(flops=0, transcendentals=0, bytes_accessed=rows * hidden * 2),
        name="pack",
    )(jnp.stack([seq_at, own, send]), w_proj, tail, w_in)


def spread_kernel(piece_ref, weight_ref, out_ref, sum_ref):
    @pl.when((pl.program_id(0) == 0) & (pl.program_id(1) == 0))
    def _():
        sum_ref[...] = jnp.zeros_like(sum_ref)

    total = sum_ref[...]
    wide = piece_ref.shape[2]
    for quarter in range(4):
        columns = slice(quarter * wide, (quarter + 1) * wide)
        piece = piece_ref[quarter].astype(jnp.float32)
        out_ref[:, columns] = piece
        product = piece * weight_ref[:, columns].astype(jnp.float32)
        for lane in range(0, wide, LANES):
            total = total + product[:, lane : lane + LANES]
    sum_ref[...] = total


def spread(pieces, weight, groups, wide):
    rows = weight.shape[0]
    per_group = weight.shape[1] // groups // (4 * wide)
    return pl.pallas_call(
        spread_kernel,
        grid=(groups, per_group),
        in_specs=[
            pl.BlockSpec((4, rows, wide), lambda g, f: (g, 0, f)),
            pl.BlockSpec((rows, 4 * wide), lambda g, f: (0, g * per_group + f)),
        ],
        out_specs=[
            pl.BlockSpec((rows, 4 * wide), lambda g, f: (0, g * per_group + f)),
            pl.BlockSpec((rows, LANES), lambda g, f: (0, 0)),
        ],
        out_shape=[
            jax.ShapeDtypeStruct(weight.shape, jnp.float32),
            jax.ShapeDtypeStruct((rows, LANES), jnp.float32),
        ],
        compiler_params=pltpu.CompilerParams(vmem_limit_bytes=32 * 2**20),
        cost_estimate=pl.CostEstimate(
            flops=weight.size * 2, transcendentals=0, bytes_accessed=weight.size * 8
        ),
        name="spread",
    )(pieces, weight)


def inverse_norm(values):
    return lax.rsqrt(jnp.mean(values * values, axis=-1, keepdims=True) + epsilon)


def norm_back(values, factor, grad_normed):
    normed = values * factor
    inner_mean = jnp.mean(grad_normed * normed, axis=-1, keepdims=True)
    return factor * (grad_normed - normed * inner_mean)


def swap_with(values, axis, bit):
    size = lax.axis_size(axis)
    return lax.ppermute(values, axis, [(i, i ^ bit) for i in range(size)])


def swapped(flag, first, second):
    return jnp.where(flag, second, first), jnp.where(flag, first, second)


def line_gather(block, axis):
    size = lax.axis_size(axis)
    index = lax.axis_index(axis)
    rows = block.shape[0]
    rising, falling = [], []
    up = down = block
    for _ in range(size - 1):
        up = lax.ppermute(up, axis, [(i, i + 1) for i in range(size - 1)])
        down = lax.ppermute(down, axis, [(i + 1, i) for i in range(size - 1)])
        rising.append(up)
        falling.append(down)
    ordered = jnp.concatenate(rising[::-1] + [block] + falling, axis=0)
    return lax.dynamic_slice_in_dim(ordered, (size - 1 - index) * rows, size * rows, 0)


def line_scatter(partial_rows, axis):
    size = lax.axis_size(axis)
    index = lax.axis_index(axis)
    rows = partial_rows.shape[0] // size

    def part(at):
        return lax.dynamic_slice_in_dim(
            partial_rows, jnp.clip(at, 0, size - 1) * rows, rows, 0
        ).astype(jnp.float32)

    up = down = None
    for step in range(1, size):
        far = size - step
        above, below = part(index + far), part(index - far)
        if up is not None:
            above, below = above + up, below + down
        up = lax.ppermute(
            above.astype(jnp.bfloat16), axis, [(i, i + 1) for i in range(size - 1)]
        ).astype(jnp.float32)
        down = lax.ppermute(
            below.astype(jnp.bfloat16), axis, [(i + 1, i) for i in range(size - 1)]
        ).astype(jnp.float32)
    return part(index) + up + down


def sum_everywhere(values, axes):
    for axis in axes:
        bit = 1
        while bit < lax.axis_size(axis):
            values = values + swap_with(values, axis, bit)
            bit *= 2
    return values


def added(first, second):
    return (first.astype(jnp.float32) + second.astype(jnp.float32)).astype(jnp.bfloat16)


def plane_gather(block):
    pairs = lax.axis_size("fsdp") // 2
    if pairs == 4:
        half = block.shape[0] // 2
        beside = swap_with(block, "fsdp", 2)
        across = swap_with(block, "fsdp", 4)
        corner = [swap_with(beside[:half], "fsdp", 4), swap_with(across[half:], "fsdp", 2)]
        return [block, beside, across, jnp.concatenate(corner, axis=0)]
    parts = [block]
    bit = 2
    while bit < 2 * pairs:
        moved = swap_with(jnp.stack(parts), "fsdp", bit)
        parts = parts + [moved[i] for i in range(len(parts))]
        bit *= 2
    return parts


def plane_scatter(parts):
    if len(parts) == 4:
        own, beside, across, corner = parts
        half = own.shape[0] // 2
        from_beside = swap_with(corner[:half], "fsdp", 2)
        from_across = swap_with(corner[half:], "fsdp", 4)
        across = jnp.concatenate([added(across[:half], from_beside), across[half:]], axis=0)
        beside = jnp.concatenate([beside[:half], added(beside[half:], from_across)], axis=0)
        beside = swap_with(beside, "fsdp", 2)
        across = swap_with(across, "fsdp", 4)
        total = own.astype(jnp.float32) + beside.astype(jnp.float32) + across.astype(jnp.float32)
        return total.astype(jnp.bfloat16)
    while len(parts) > 1:
        half = len(parts) // 2
        moved = swap_with(jnp.stack(parts[half:]), "fsdp", 2 * half)
        parts = [added(parts[i], moved[i]) for i in range(half)]
    return parts[0]


def in_order(parts, place):
    count = len(parts)
    bit = 1
    while bit < count:
        flag = (place // bit) % 2 == 1
        parts = [jnp.where(flag, parts[k ^ bit], parts[k]) for k in range(count)]
        bit *= 2
    return parts


def group_gather(block):
    along = swap_with(block, "seq", 1)
    return [block, swap_with(block, "fsdp", 1), along, swap_with(along, "fsdp", 1)]


def group_scatter(parts):
    sent = swap_with(jnp.concatenate([parts[1], parts[3]], axis=0), "fsdp", 1)
    rows = parts[0].shape[0]
    own = parts[0].astype(jnp.float32) + sent[:rows].astype(jnp.float32)
    along = added(parts[2], sent[rows:])
    return own + swap_with(along, "seq", 1).astype(jnp.float32)


def body(
    inputs,
    norm_attn,
    w_proj,
    w_small,
    forget_bias,
    qk_gain,
    w_out,
    norm_ffn,
    w_in,
    w_down,
    cotangent,
):
    row_count, model_width = inputs.shape
    weight_rows = w_proj.shape[0]
    seq_parts = lax.axis_size("seq")
    fsdp_parts = lax.axis_size("fsdp")
    seq_at = lax.axis_index("seq")
    fsdp_at = lax.axis_index("fsdp")
    core = fsdp_at % 2
    place = fsdp_at // 2
    places = fsdp_parts // 2
    chip_rows = 2 * weight_rows
    quarter = 2 * (seq_at % 2) + core
    head_count = forget_bias.shape[0]
    head_width = qk_gain.shape[1]
    heads = head_count // seq_parts
    wide = heads * head_width
    small_wide = 3 * heads
    quarter_rows = w_down.shape[0] // 4
    hidden = fsdp_parts * quarter_rows

    every_input = line_gather(inputs, "seq")
    local_small = lax.dynamic_index_in_dim(
        w_small.reshape(weight_rows, 3, seq_parts, heads), seq_at, 2, False
    ).reshape(weight_rows, small_wide)
    tail = jnp.concatenate(
        [
            local_small,
            norm_attn[:, None],
            norm_ffn[:, None],
            jnp.zeros((weight_rows, LANES - small_wide - 2), jnp.bfloat16),
        ],
        axis=1,
    )
    packed, own_in, send_in = pack(
        w_proj, tail, w_in, seq_at, quarter, quarter ^ 1, seq_parts, quarter_rows
    )
    packed_full = lax.all_gather(packed, "fsdp", axis=0, tiled=True)
    gain_attention = packed_full[:, 4 * wide + small_wide].astype(jnp.float32)
    gain_ffn = packed_full[:, 4 * wide + small_wide + 1].astype(jnp.float32)
    out_full = lax.all_gather(w_out, "fsdp", axis=0, tiled=True)

    def chip_block(own, send):
        return jnp.concatenate(swapped(core == 1, own, swap_with(send, "fsdp", 1)), axis=0)

    in_parts = plane_gather(chip_block(own_in, send_in))
    in_full = jnp.concatenate(in_parts, axis=0)
    own_down = lax.dynamic_slice_in_dim(w_down, quarter * quarter_rows, quarter_rows, 0)
    send_down = lax.dynamic_slice_in_dim(w_down, (quarter ^ 1) * quarter_rows, quarter_rows, 0)
    down_parts = plane_gather(chip_block(own_down, send_down))
    down_full = jnp.concatenate(in_order(down_parts, place), axis=0)

    late_cotangent, every_input = lax.optimization_barrier((cotangent, every_input))
    cotangent_group = jnp.concatenate(group_gather(late_cotangent), axis=0)

    wide_input = every_input.astype(jnp.float32)
    normed = (wide_input * inverse_norm(wide_input) * gain_attention).astype(jnp.bfloat16)
    projected = dot_ab(normed, packed_full).astype(jnp.bfloat16)
    bias_lanes = jnp.repeat(
        lax.dynamic_slice_in_dim(forget_bias, seq_at * heads, heads, 0), head_width
    ).reshape(heads // 2, 1, LANES)
    gain_lanes = jnp.tile(qk_gain.astype(jnp.float32), (1, 2))
    gated, attended, shift = attend(projected, bias_lanes, gain_lanes, heads)
    mixed_rows = lax.all_to_all(gated, "seq", split_axis=0, concat_axis=1, tiled=True)

    def features_by_place(values):
        blocks = [values[:, k * chip_rows : (k + 1) * chip_rows] for k in range(places)]
        return jnp.concatenate(in_order(blocks, place), axis=1)

    source = inputs.astype(jnp.float32)
    residual = source + dot_ab(mixed_rows, out_full)
    factor_ffn = inverse_norm(residual)
    normed_ffn = (residual * factor_ffn * gain_ffn).astype(jnp.bfloat16)
    normed_group = jnp.concatenate(group_gather(features_by_place(normed_ffn)), axis=0)
    gate_up = dot_ab(normed_group, in_full)
    gate_part = gate_up[:, :hidden]
    up_part = gate_up[:, hidden:]
    inner_sigmoid = jax.nn.sigmoid(gate_part)
    silu_gate = gate_part * inner_sigmoid
    activated = (silu_gate * up_part).astype(jnp.bfloat16)

    def by_rows(values):
        values = values.astype(jnp.bfloat16)
        return [values[k * row_count : (k + 1) * row_count] for k in range(4)]

    output = (residual + group_scatter(by_rows(dot_ab(activated, down_full)))).astype(jnp.bfloat16)

    grad_act = dot_abt(cotangent_group, down_full)
    grad_gate = grad_act * up_part * inner_sigmoid * (1.0 + gate_part * (1.0 - inner_sigmoid))
    grad_up = grad_act * silu_gate
    grad_gate_up = jnp.concatenate([grad_gate, grad_up], axis=1).astype(jnp.bfloat16)
    grad_normed_ffn = features_by_place(group_scatter(by_rows(dot_abt(grad_gate_up, in_full))))
    grad_residual = cotangent.astype(jnp.float32) + norm_back(
        residual, factor_ffn, grad_normed_ffn * gain_ffn
    )
    grad_branch = grad_residual.astype(jnp.bfloat16)
    grad_mixed = dot_abt(grad_branch, out_full).astype(jnp.bfloat16)
    grad_heads = lax.all_to_all(grad_mixed, "seq", split_axis=1, concat_axis=0, tiled=True)

    grad_in = dot_atb(normed_group, grad_gate_up).astype(jnp.bfloat16)
    grad_down = dot_atb(activated, cotangent_group).astype(jnp.bfloat16)
    grad_out = dot_atb(mixed_rows, grad_branch).astype(jnp.bfloat16)
    grad_in = plane_scatter([grad_in[k * chip_rows : (k + 1) * chip_rows] for k in range(places)])
    grad_down = grad_down.reshape(places, 2 * quarter_rows, model_width)
    grad_down = plane_scatter(
        [lax.dynamic_index_in_dim(grad_down, place ^ k, 0, False) for k in range(places)]
    )

    def both_quarters(block):
        rows = block.shape[0] // 2
        own = lax.dynamic_slice_in_dim(block, core * rows, rows, 0)
        sent = lax.dynamic_slice_in_dim(block, (1 - core) * rows, rows, 0)
        return jnp.stack(swapped(core == 1, own, swap_with(sent, "fsdp", 1)))

    far = seq_at >= 2

    def all_pieces(first, second):
        keep, send = swapped(far, first, second)
        return line_gather(added(keep, swap_with(send, "seq", 2))[None], "seq")

    grad_in = both_quarters(grad_in)
    grad_in = all_pieces(grad_in[:, :, :hidden], grad_in[:, :, hidden:])
    grad_down = both_quarters(grad_down)
    grad_down = all_pieces(
        grad_down[:, : quarter_rows // 2], grad_down[:, quarter_rows // 2 :]
    )
    grad_down = (
        grad_down.reshape(2, 2, 2, quarter_rows // 2, model_width)
        .transpose(1, 2, 0, 3, 4)
        .reshape(4 * quarter_rows, model_width)
        .astype(jnp.float32)
    )
    grad_out = lax.psum_scatter(grad_out, "fsdp", scatter_dimension=0, tiled=True)
    grad_out = lax.psum(grad_out, "seq").astype(jnp.float32)

    grad_projected, gain_sums, forget_sums = attend_back(
        projected, bias_lanes, gain_lanes, attended, shift, grad_heads, heads
    )
    grad_packed = dot_atb(normed, grad_projected).astype(jnp.bfloat16)
    grad_packed = grad_packed.reshape(places, 2, weight_rows, 4 * wide + LANES)
    grad_packed = added(
        lax.dynamic_index_in_dim(grad_packed, core, 1, False),
        swap_with(lax.dynamic_index_in_dim(grad_packed, 1 - core, 1, False), "fsdp", 1),
    )
    grad_packed = plane_scatter(
        [lax.dynamic_index_in_dim(grad_packed, place ^ k, 0, False) for k in range(places)]
    )
    every_packed = line_gather(grad_packed[None], "seq")
    grad_normed = line_scatter(dot_abt(grad_projected, packed_full).astype(jnp.bfloat16), "seq")
    grad_inputs = grad_residual + norm_back(
        source, inverse_norm(source), grad_normed * gain_attention
    )

    bias_row = lax.dynamic_update_slice_in_dim(
        jnp.zeros((LANES,), jnp.float32),
        forget_sums.reshape(heads, head_width)[:, 0],
        seq_at * heads,
        0,
    )
    sums = sum_everywhere(jnp.concatenate([gain_sums, bias_row[None]], axis=0), ("fsdp", "seq"))
    grad_qk_gain = sums[:2, :head_width] + sums[:2, head_width:]
    grad_forget_bias = sums[2, :head_count]

    grad_small = jnp.moveaxis(
        every_packed[:, :, 4 * wide : 4 * wide + small_wide]
        .astype(jnp.float32)
        .reshape(seq_parts, weight_rows, 3, heads),
        0,
        2,
    ).reshape(weight_rows, 3 * head_count)
    if quarter_rows % LANES or wide % LANES:
        folded = grad_in.reshape(2, 4, weight_rows, fsdp_parts, quarter_rows)
        grad_in = folded.transpose(2, 0, 3, 1, 4).reshape(w_in.shape).astype(jnp.float32)
        folded = every_packed[:, :, : 4 * wide].reshape(seq_parts, weight_rows, 4, wide)
        grad_proj = folded.transpose(1, 2, 0, 3).reshape(w_proj.shape).astype(jnp.float32)
        in_sums = grad_in * w_in.astype(jnp.float32)
        proj_sums = grad_proj * w_proj.astype(jnp.float32)
    else:
        grad_in, in_sums = spread(
            grad_in.reshape(8, weight_rows, hidden), w_in, 2, quarter_rows
        )
        grad_proj, proj_sums = spread(every_packed, w_proj, 1, wide)
    grad_gain_attention = (
        jnp.sum(proj_sums, axis=1)
        + jnp.sum(grad_small * w_small.astype(jnp.float32), axis=1)
    ) / norm_attn.astype(jnp.float32)
    grad_gain_ffn = jnp.sum(in_sums, axis=1) / norm_ffn.astype(jnp.float32)
    return (
        output,
        grad_inputs,
        grad_gain_attention,
        grad_proj,
        grad_small,
        grad_forget_bias,
        grad_qk_gain,
        grad_out,
        grad_gain_ffn,
        grad_in,
        grad_down,
    )


def solution(mesh):
    in_specs = (
        P(("fsdp", "seq"), None),
        P("fsdp"),
        P("fsdp", None),
        P("fsdp", None),
        P(),
        P(),
        P("fsdp", None),
        P("fsdp"),
        P("fsdp", None),
        P("fsdp", None),
        P(("fsdp", "seq"), None),
    )
    out_specs = (
        P(("fsdp", "seq"), None),
        P(("fsdp", "seq"), None),
        P("fsdp"),
        P("fsdp", None),
        P("fsdp", None),
        P(),
        P(),
        P("fsdp", None),
        P("fsdp"),
        P("fsdp", None),
        P("fsdp", None),
    )
    return jax.shard_map(body, mesh=mesh, in_specs=in_specs, out_specs=out_specs, check_vma=False)
```
